32 devices in a mesh: gx: 8 (over y, x, core), gy: 4 (over z).
Axes of the slice: x: 2, y: 2, z: 4, core: 2. Of those that a mesh axis runs over, the one named last changes fastest.
Arguments:
- field: float32 [65536, 512], P(('gx', 'gy')), may hold values from -6 to 6
Outputs:
- spectrum: float32 [65536, 512], P('gx', 'gy')
The draws below stay inside these ranges and needn't reach their ends.
All inputs are finite; a program needn't handle non-finite values.
Results may differ from the reference program's by a relative error of at most 0.00007.
Values sent between devices are 32-bit elements; how exact they have to be, the bound alone decides.
A program may use at most 64 MiB of HBM per device.

```python
import math
import jax
import jax.numpy as jnp
from jax import lax

P_SIZE = 256
Q = 256
LENGTH = 65536
COLUMNS = 512


def steps_of(stream_key, dims, shards, least, largest):
    level = 1.0
    for axis_at, blocks in shards:
        draws = jax.random.uniform(jax.random.fold_in(jax.random.fold_in(stream_key, 6), axis_at), (blocks,), jnp.float32, least / len(shards), largest / len(shards))
        level = level * jnp.repeat(jnp.exp(draws), dims[axis_at] // blocks).reshape((-1,) + (1,) * (len(dims) - 1 - axis_at))
    return level


def bell_draw(rng, dims, width, limit, shards=(), kind=jnp.bfloat16):
    values = width * jax.random.normal(rng, dims, jnp.float32)
    if shards:
        values = values * steps_of(rng, dims, shards, -0.22, 0.18)
    return jnp.clip(values, -limit, limit).astype(kind)


def setup_inputs(seed: int = 0) -> dict:
    splits = jax.random.split(jax.random.key(seed), 2)
    field = bell_draw(splits[0], (LENGTH, COLUMNS), 1.0, 6.0, ((0, 32),), jnp.float32)
    return {"field": field}


def one_block(columns):
    length = P_SIZE * Q
    reordered = jnp.concatenate([columns[0::2], columns[1::2][::-1]], axis=0)
    fourier = jnp.fft.fft(reordered, axis=0)
    indices = jnp.arange(length).astype(jnp.float32)
    phases = math.pi / (2.0 * length) * indices
    factor = math.sqrt(2.0 / length)
    result = factor * (jnp.cos(phases)[:, None] * jnp.real(fourier) + jnp.sin(phases)[:, None] * jnp.imag(fourier))
    return result.astype(jnp.float32)

def reference(field):
    length = P_SIZE * Q
    block_width = math.gcd(COLUMNS, 128)
    count_blocks = COLUMNS // block_width
    stacked = jnp.transpose(field.reshape(length, count_blocks, block_width), (1, 0, 2))
    mapped = lax.map(one_block, stacked)
    return jnp.transpose(mapped, (1, 0, 2)).reshape(length, COLUMNS)
```

```python
import functools
import math

import jax
import jax.numpy as jnp
import numpy as np
from jax import lax
from jax.experimental import pallas as pl
from jax.experimental.pallas import tpu as pltpu
from jax.sharding import PartitionSpec as P

P_SIZE = 256
Q = 256
HALF = P_SIZE // 2
LANES = 128
STEP = 4

MESH = pl.DeviceIdType.MESH
highest = lax.Precision.HIGHEST


def mat_dot(left, right):
    return jnp.dot(left, right, precision=highest, preferred_element_type=jnp.float32)


def finish(spec_real, spec_imag, frequency):
    length = P_SIZE * Q
    phases = math.pi / (2.0 * length) * frequency.astype(jnp.float32)
    factor = math.sqrt(2.0 / length)
    return factor * (
        jnp.cos(phases)[:, :, None] * spec_real + jnp.sin(phases)[:, :, None] * spec_imag
    )


def body(field):
    groups = lax.axis_size("gx")
    position = lax.axis_index("gx")
    length = P_SIZE * Q
    joined = lax.all_to_all(field, "gy", split_axis=1, concat_axis=0, tiled=True)
    row_count = joined.shape[0]
    col_width = joined.shape[1]
    half_rows = P_SIZE // (2 * groups)
    local_q = Q // groups
    local_p = P_SIZE // groups
    paired = joined.reshape(row_count // 2, 2, col_width)
    even_rows = paired[:, 0].reshape(half_rows, Q, col_width)
    odd_rows = jnp.flip(paired[:, 1].reshape(half_rows, Q, col_width), axis=1)
    low_half, high_half = (
        lax.all_to_all(even_rows, "gx", split_axis=1, concat_axis=0, tiled=True),
        lax.all_to_all(odd_rows, "gx", split_axis=1, concat_axis=0, tiled=True),
    )
    freq_first = jnp.arange(P_SIZE, dtype=jnp.int32)
    place_low = jnp.arange(P_SIZE // 2, dtype=jnp.int32)
    place_high = P_SIZE - 1 - place_low
    two_pi = 2.0 * math.pi
    low_phase = (
        two_pi / P_SIZE * (freq_first[:, None] * place_low[None, :] % P_SIZE).astype(jnp.float32)
    )
    high_phase = (
        two_pi / P_SIZE * (freq_first[:, None] * place_high[None, :] % P_SIZE).astype(jnp.float32)
    )
    flat_low = low_half.reshape(P_SIZE // 2, local_q * col_width)
    flat_high = high_half.reshape(P_SIZE // 2, local_q * col_width)
    cos_part = (
        mat_dot(jnp.cos(low_phase), flat_low) + mat_dot(jnp.cos(high_phase), flat_high)
    ).reshape(P_SIZE, local_q, col_width)
    sin_part = (
        mat_dot(jnp.sin(low_phase), flat_low) + mat_dot(jnp.sin(high_phase), flat_high)
    ).reshape(P_SIZE, local_q, col_width)
    part_imag = -sin_part
    second_place = position * local_q + jnp.arange(local_q, dtype=jnp.int32)
    turn_phase = (
        two_pi / length * (freq_first[:, None] * second_place[None, :] % length).astype(jnp.float32)
    )
    turn_cos = jnp.cos(turn_phase)[:, :, None]
    turn_sin = jnp.sin(turn_phase)[:, :, None]
    turned_real = cos_part * turn_cos + part_imag * turn_sin
    turned_imag = part_imag * turn_cos - cos_part * turn_sin
    moved_real, moved_imag = (
        lax.all_to_all(turned_real, "gx", split_axis=0, concat_axis=1, tiled=True),
        lax.all_to_all(turned_imag, "gx", split_axis=0, concat_axis=1, tiled=True),
    )
    second_index = jnp.arange(Q, dtype=jnp.int32)
    row_phase = two_pi / Q * (second_index[:, None] * second_index[None, :] % Q).astype(jnp.float32)
    row_cos = jnp.cos(row_phase)
    row_sin = jnp.sin(row_phase)
    spec_real = jnp.einsum("jb,kbc->jkc", row_cos, moved_real, precision=highest) + jnp.einsum(
        "jb,kbc->jkc", row_sin, moved_imag, precision=highest
    )
    spec_imag = jnp.einsum("jb,kbc->jkc", row_cos, moved_imag, precision=highest) - jnp.einsum(
        "jb,kbc->jkc", row_sin, moved_real, precision=highest
    )
    block_rows = lax.dynamic_slice_in_dim(freq_first, position * local_p, local_p, 0)
    frequency = block_rows[None, :] + P_SIZE * second_index[:, None]
    result = finish(spec_real, spec_imag, frequency)
    arrived = lax.all_to_all(result, "gx", split_axis=0, concat_axis=1, tiled=True)
    return arrived.reshape(local_q * P_SIZE, col_width)


def split_np(table):
    high = table.astype(jnp.bfloat16)
    low = (table - high.astype(np.float64)).astype(jnp.bfloat16)
    return np.stack([high, low])


def order_of_q(groups):
    pairs = HALF // groups
    order = []
    for group in range(groups):
        for start in range(0, pairs, STEP):
            low = [group * pairs + start + i for i in range(STEP)]
            order += low + [Q - 1 - q for q in low]
    return np.array(order)


def first_matrix():
    low = np.arange(HALF)
    place = np.concatenate([low, P_SIZE - 1 - low])
    angle = 2 * np.pi / P_SIZE * (low[:, None] * place[None, :] % P_SIZE)
    real, imag = np.cos(angle), -np.sin(angle)
    imag[0] = np.cos(np.pi * place)
    return split_np(np.concatenate([real, imag]))


def second_matrices(groups):
    length = P_SIZE * Q
    q = order_of_q(groups)[None, :]
    k2 = np.arange(Q)[:, None]
    angle = 2 * np.pi / Q * (k2 * q % Q)
    usual = np.concatenate([np.cos(angle), np.sin(angle)])
    factor = math.sqrt(2.0 / length)
    def row(k):
        return factor * np.cos(2 * np.pi / (4 * length) * (k * (4 * q + 1) % (4 * length)))
    special = np.concatenate([row(P_SIZE * k2), row(HALF + P_SIZE * (Q - 1 - k2))])
    return np.stack([split_np(usual), split_np(special)])


def split(value):
    high = value.astype(jnp.bfloat16)
    low = (value - high.astype(jnp.float32)).astype(jnp.bfloat16)
    return high, low


def three_dots(high, low, value):
    value_high, value_low = split(value)
    dot = functools.partial(jnp.dot, preferred_element_type=jnp.float32)
    return dot(high, value_high) + (dot(high, value_low) + dot(low, value_high))


def kernel(
    groups, planes, x_ref, first_ref, second_ref, out_ref,
    got_rows, part, got_part, coef, turn_cos, turn_sin, end_cos, end_sin,
    recv_rows, send_rows, recv_part, send_part, recv_coef, send_coef,
):
    gx, gy = lax.axis_index("gx"), lax.axis_index("gy")
    devices = groups * planes
    length = P_SIZE * Q
    pairs = HALF // groups
    chunks = pairs // STEP
    own = x_ref.shape[0]
    width = 2 * STEP
    block = Q // groups

    barrier = pltpu.get_barrier_semaphore()

    def target(offset):
        return lax.rem(gx + offset // planes, groups), lax.rem(gy + offset % planes, planes)

    def greet(offset, carry):
        pl.semaphore_signal(barrier, inc=1, device_id=target(offset), device_id_type=MESH)
        return carry

    lax.fori_loop(1, devices, greet, 0)
    pl.semaphore_wait(barrier, devices - 1)

    first_place = (gx * planes + gy) * own

    def row_copies(chunk, gxd, gyd):
        low = pl.multiple_of((gxd * pairs + chunk * STEP) * 2, width)
        high = pl.multiple_of(2 * Q - (gxd * pairs + (chunk + 1) * STEP) * 2, width)
        columns = pl.ds(pl.multiple_of(gyd * LANES, LANES), LANES)
        for side, at in ((0, low), (1, high)):
            yield (
                x_ref.at[:, pl.ds(at, width), columns],
                got_rows.at[chunk, pl.ds(first_place, own), pl.ds(side * width, width), :],
            )

    def send_chunk(chunk, carry):
        for source, place in row_copies(chunk, gx, gy):
            pltpu.make_async_copy(source, place, recv_rows.at[chunk]).start()

        def send(offset, carry):
            gxd, gyd = target(offset)
            for source, place in row_copies(chunk, gxd, gyd):
                pltpu.make_async_remote_copy(
                    src_ref=source, dst_ref=place, send_sem=send_rows,
                    recv_sem=recv_rows.at[chunk], device_id=(gxd, gyd), device_id_type=MESH,
                ).start()
            return carry

        lax.fori_loop(1, devices, send, 0)
        return carry

    lax.fori_loop(0, chunks, send_chunk, 0)

    slot_row = lax.broadcasted_iota(jnp.int32, (HALF, LANES), 0)

    def turn_table(at, carry):
        chunk, inner = at // width, at % width
        base = gx * pairs + chunk * STEP
        q = jnp.where(inner < STEP, base + inner, Q - 1 - (base + inner - STEP))
        angle = (slot_row * q).astype(jnp.float32) * (2 * math.pi / length)
        turn_cos[at] = jnp.cos(angle)
        turn_sin[at] = jnp.sin(angle)
        return carry

    lax.fori_loop(0, 2 * pairs, turn_table, 0)
    k2_row = lax.broadcasted_iota(jnp.int32, (Q, LANES), 0)
    end_angle = k2_row.astype(jnp.float32) * (math.pi * P_SIZE / (2 * length))
    factor = math.sqrt(2.0 / length)
    end_cos[...] = factor * jnp.cos(end_angle)
    end_sin[...] = factor * jnp.sin(end_angle)

    def first_stage(chunk, carry):
        rows = got_rows.at[chunk]
        pltpu.make_async_copy(rows, rows, recv_rows.at[chunk]).wait()
        flat = rows.reshape(HALF * 2 * width, LANES)

        def line(row):
            return flat[pl.ds(row, HALF, stride=2 * width), :]

        for i in range(STEP):
            mirror = width + 2 * (STEP - 1 - i)
            value = jnp.concatenate(
                [
                    jnp.concatenate([line(2 * i), line(mirror)], axis=1),
                    jnp.concatenate([line(mirror + 1), line(2 * i + 1)], axis=1),
                ],
                axis=0,
            )
            both = three_dots(first_ref[0], first_ref[1], value)
            for side in range(2):
                inner = side * STEP + i
                real = both[:HALF, side * LANES : (side + 1) * LANES]
                imag = both[HALF:, side * LANES : (side + 1) * LANES]
                cos = turn_cos[chunk * width + inner]
                sin = turn_sin[chunk * width + inner]
                turned = real * cos + imag * sin, imag * cos - real * sin
                for plane in range(2):
                    part[chunk, :, inner, plane] = turned[plane].reshape(groups, pairs, LANES)

        pltpu.make_async_copy(part.at[chunk, gx], got_part.at[gx, chunk], recv_part).start()
        for offset in range(1, groups):
            other = lax.rem(gx + offset, groups)
            pltpu.make_async_remote_copy(
                src_ref=part.at[chunk, other], dst_ref=got_part.at[gx, chunk],
                send_sem=send_part, recv_sem=recv_part,
                device_id=(other, gy), device_id_type=MESH,
            ).start()
        return carry

    lax.fori_loop(0, chunks, first_stage, 0)
    pltpu.make_async_copy(got_part, got_part, recv_part).wait()

    flat_part = got_part.reshape(Q * 2 * pairs, LANES)
    flat_coef = coef.reshape(2 * Q * pairs, LANES)
    eight = 8

    def second_stage(slot, carry):
        value = jnp.concatenate(
            [
                flat_part[pl.ds(plane * pairs + slot, Q, stride=2 * pairs), :]
                for plane in range(2)
            ],
            axis=1,
        )
        frequency = gx * pairs + slot
        alone = frequency == 0
        which = jnp.where(alone, 1, 0)
        product = three_dots(second_ref[which, 0], second_ref[which, 1], value)
        top_real, top_imag = product[:Q, :LANES], product[:Q, LANES:]
        low_real, low_imag = product[Q:, :LANES], product[Q:, LANES:]
        spec_real = top_real + low_imag
        spec_imag = top_imag - low_real
        angle = jnp.full((8, LANES), frequency, jnp.int32).astype(jnp.float32) * (
            math.pi / (2 * length)
        )
        cos_one, sin_one = jnp.cos(angle)[:1], jnp.sin(angle)[:1]
        cos = end_cos[...] * cos_one - end_sin[...] * sin_one
        sin = end_sin[...] * cos_one + end_cos[...] * sin_one
        near = jnp.where(alone, top_real, cos * spec_real + sin * spec_imag)
        far = jnp.where(alone, low_imag, sin * spec_real - cos * spec_imag)
        flat_coef[pl.ds(slot, Q, stride=pairs), :] = near
        flat_coef[pl.ds(Q * pairs + pairs - 1 - slot, Q, stride=pairs), :] = far
        return carry

    def coef_copies(step, other):
        near = step * eight
        far = pairs - eight - near
        yield (
            coef.at[0, pl.ds(pl.multiple_of(other * block, block), block), pl.ds(near, eight)],
            out_ref.at[0, :, pl.ds(pl.multiple_of(gx * pairs + near, eight), eight)],
        )
        away = groups - 1 - other
        yield (
            coef.at[1, pl.ds(pl.multiple_of(away * block, block), block), pl.ds(far, eight)],
            out_ref.at[1, :, pl.ds(pl.multiple_of((groups - 1 - gx) * pairs + far, eight), eight)],
        )

    for step in range(pairs // eight):
        lax.fori_loop(step * eight, (step + 1) * eight, second_stage, 0)
        for source, place in coef_copies(step, gx):
            pltpu.make_async_copy(source, place, recv_coef).start()
        for offset in range(1, groups):
            other = lax.rem(gx + offset, groups)
            for source, place in coef_copies(step, other):
                pltpu.make_async_remote_copy(
                    src_ref=source, dst_ref=place, send_sem=send_coef, recv_sem=recv_coef,
                    device_id=(other, gy), device_id_type=MESH,
                ).start()

    pltpu.make_async_copy(out_ref, out_ref, recv_coef).wait()
    sent = x_ref.at[:, pl.ds(0, 2 * Q - 2 * Q // devices), :]
    pltpu.make_async_copy(sent, sent, send_rows).wait()
    sent = part.at[:, pl.ds(0, groups - 1)]
    pltpu.make_async_copy(sent, sent, send_part).wait()
    sent = coef.at[:, pl.ds(0, Q - block)]
    pltpu.make_async_copy(sent, sent, send_coef).wait()


def fused_body(field):
    groups, planes = lax.axis_size("gx"), lax.axis_size("gy")
    pairs = HALF // groups
    chunks = pairs // STEP
    block = Q // groups
    own = field.shape[0] // (2 * Q)
    width = 2 * STEP
    f32 = jnp.float32
    vmem = pl.BlockSpec(memory_space=pltpu.VMEM)
    dma = pltpu.SemaphoreType.DMA
    both = pl.pallas_call(
        functools.partial(kernel, groups, planes),
        out_shape=jax.ShapeDtypeStruct((2, block, HALF, LANES), f32),
        in_specs=[pl.BlockSpec(memory_space=pl.ANY), vmem, vmem],
        out_specs=vmem,
        scratch_shapes=[
            pltpu.VMEM((chunks, HALF, 2 * width, LANES), f32),
            pltpu.VMEM((chunks, groups, width, 2, pairs, LANES), f32),
            pltpu.VMEM((groups, chunks, width, 2, pairs, LANES), f32),
            pltpu.VMEM((2, Q, pairs, LANES), f32),
            pltpu.VMEM((2 * pairs, HALF, LANES), f32),
            pltpu.VMEM((2 * pairs, HALF, LANES), f32),
            pltpu.VMEM((Q, LANES), f32),
            pltpu.VMEM((Q, LANES), f32),
            dma((chunks,)), dma, dma, dma, dma, dma,
        ],
        compiler_params=pltpu.CompilerParams(
            collective_id=0, has_side_effects=True, vmem_limit_bytes=48 * 1024 * 1024
        ),
    )(
        field.reshape(own, 2 * Q, field.shape[1]),
        jnp.asarray(first_matrix()),
        jnp.asarray(second_matrices(groups)),
    )
    far = both[1, ::-1]
    result = jnp.concatenate([both[0], far[:, HALF - 1 :], far[:, : HALF - 1]], axis=1)
    return result.reshape(block * P_SIZE, LANES)


def fits(mesh):
    groups, planes = mesh.shape["gx"], mesh.shape["gy"]
    pairs = HALF // groups
    return pairs % 8 == 0 and (P_SIZE * Q) % (groups * planes * 2 * Q) == 0


def solution(mesh):
    in_specs = (P(("gx", "gy"), None),)
    out_specs = P("gx", "gy")
    def run(field):
        fused = fits(mesh) and field.shape[1] == LANES * mesh.shape["gy"]
        chosen = fused_body if fused else body
        return jax.shard_map(
            chosen, mesh=mesh, in_specs=in_specs, out_specs=out_specs, check_vma=False
        )(field)
    return run
```

```python
import functools
import math

import jax
import jax.numpy as jnp
import numpy as np
from jax import lax
from jax.experimental import pallas as pl
from jax.experimental.pallas import tpu as pltpu
from jax.sharding import PartitionSpec as P

P_SIZE = 256
Q = 256
HALF = P_SIZE // 2
LANES = 128
STEP = 4
EIGHT = 8

MESH = pl.DeviceIdType.MESH
highest = lax.Precision.HIGHEST


def mat_dot(left, right):
    return jnp.dot(left, right, precision=highest, preferred_element_type=jnp.float32)


def finish(spec_real, spec_imag, frequency):
    length = P_SIZE * Q
    phases = math.pi / (2.0 * length) * frequency.astype(jnp.float32)
    factor = math.sqrt(2.0 / length)
    return factor * (
        jnp.cos(phases)[:, :, None] * spec_real + jnp.sin(phases)[:, :, None] * spec_imag
    )


def body(field):
    groups = lax.axis_size("gx")
    position = lax.axis_index("gx")
    length = P_SIZE * Q
    joined = lax.all_to_all(field, "gy", split_axis=1, concat_axis=0, tiled=True)
    row_count = joined.shape[0]
    col_width = joined.shape[1]
    half_rows = P_SIZE // (2 * groups)
    local_q = Q // groups
    local_p = P_SIZE // groups
    paired = joined.reshape(row_count // 2, 2, col_width)
    even_rows = paired[:, 0].reshape(half_rows, Q, col_width)
    odd_rows = jnp.flip(paired[:, 1].reshape(half_rows, Q, col_width), axis=1)
    low_half, high_half = (
        lax.all_to_all(even_rows, "gx", split_axis=1, concat_axis=0, tiled=True),
        lax.all_to_all(odd_rows, "gx", split_axis=1, concat_axis=0, tiled=True),
    )
    freq_first = jnp.arange(P_SIZE, dtype=jnp.int32)
    place_low = jnp.arange(P_SIZE // 2, dtype=jnp.int32)
    place_high = P_SIZE - 1 - place_low
    two_pi = 2.0 * math.pi
    low_phase = (
        two_pi / P_SIZE * (freq_first[:, None] * place_low[None, :] % P_SIZE).astype(jnp.float32)
    )
    high_phase = (
        two_pi / P_SIZE * (freq_first[:, None] * place_high[None, :] % P_SIZE).astype(jnp.float32)
    )
    flat_low = low_half.reshape(P_SIZE // 2, local_q * col_width)
    flat_high = high_half.reshape(P_SIZE // 2, local_q * col_width)
    cos_part = (
        mat_dot(jnp.cos(low_phase), flat_low) + mat_dot(jnp.cos(high_phase), flat_high)
    ).reshape(P_SIZE, local_q, col_width)
    sin_part = (
        mat_dot(jnp.sin(low_phase), flat_low) + mat_dot(jnp.sin(high_phase), flat_high)
    ).reshape(P_SIZE, local_q, col_width)
    part_imag = -sin_part
    second_place = position * local_q + jnp.arange(local_q, dtype=jnp.int32)
    turn_phase = (
        two_pi / length * (freq_first[:, None] * second_place[None, :] % length).astype(jnp.float32)
    )
    turn_cos = jnp.cos(turn_phase)[:, :, None]
    turn_sin = jnp.sin(turn_phase)[:, :, None]
    turned_real = cos_part * turn_cos + part_imag * turn_sin
    turned_imag = part_imag * turn_cos - cos_part * turn_sin
    moved_real, moved_imag = (
        lax.all_to_all(turned_real, "gx", split_axis=0, concat_axis=1, tiled=True),
        lax.all_to_all(turned_imag, "gx", split_axis=0, concat_axis=1, tiled=True),
    )
    second_index = jnp.arange(Q, dtype=jnp.int32)
    row_phase = two_pi / Q * (second_index[:, None] * second_index[None, :] % Q).astype(jnp.float32)
    row_cos = jnp.cos(row_phase)
    row_sin = jnp.sin(row_phase)
    spec_real = jnp.einsum("jb,kbc->jkc", row_cos, moved_real, precision=highest) + jnp.einsum(
        "jb,kbc->jkc", row_sin, moved_imag, precision=highest
    )
    spec_imag = jnp.einsum("jb,kbc->jkc", row_cos, moved_imag, precision=highest) - jnp.einsum(
        "jb,kbc->jkc", row_sin, moved_real, precision=highest
    )
    block_rows = lax.dynamic_slice_in_dim(freq_first, position * local_p, local_p, 0)
    frequency = block_rows[None, :] + P_SIZE * second_index[:, None]
    result = finish(spec_real, spec_imag, frequency)
    arrived = lax.all_to_all(result, "gx", split_axis=0, concat_axis=1, tiled=True)
    return arrived.reshape(local_q * P_SIZE, col_width)


def split_np(table):
    high = table.astype(jnp.bfloat16)
    low = (table - high.astype(np.float64)).astype(jnp.bfloat16)
    return np.stack([high, low])


def order_of_q(groups):
    pairs = HALF // groups
    order = []
    for group in range(groups):
        for start in range(0, pairs, STEP):
            low = [group * pairs + start + i for i in range(STEP)]
            order += low + [Q - 1 - q for q in low]
    return np.array(order)


def first_matrix():
    low = np.arange(HALF)
    place = np.concatenate([low, P_SIZE - 1 - low])
    angle = 2 * np.pi / P_SIZE * (low[:, None] * place[None, :] % P_SIZE)
    real, imag = np.cos(angle), -np.sin(angle)
    imag[0] = np.cos(np.pi * place)
    return split_np(np.concatenate([real, imag]))


def second_matrices(groups):
    length = P_SIZE * Q
    q = order_of_q(groups)[None, :]
    k2 = np.arange(Q)[:, None]
    angle = 2 * np.pi / Q * (k2 * q % Q)
    usual = np.concatenate([np.cos(angle), np.sin(angle)])
    factor = math.sqrt(2.0 / length)
    def row(k):
        return factor * np.cos(2 * np.pi / (4 * length) * (k * (4 * q + 1) % (4 * length)))
    special = np.concatenate([row(P_SIZE * k2), row(HALF + P_SIZE * (Q - 1 - k2))])
    return np.stack([split_np(usual), split_np(special)])


def split(value):
    high = value.astype(jnp.bfloat16)
    low = (value - high.astype(jnp.float32)).astype(jnp.bfloat16)
    return high, low


def three_dots(high, low, value):
    value_high, value_low = split(value)
    dot = functools.partial(jnp.dot, preferred_element_type=jnp.float32)
    return dot(high, value_high) + (dot(high, value_low) + dot(low, value_high))


def kernel(
    groups, planes, x_ref, first_hbm, second_hbm, out_ref, first_ref, second_ref,
    got_rows, part, got_part, coef, turn_cos, turn_sin, end_cos, end_sin,
    recv_rows, send_rows, recv_part, send_part, recv_coef, send_coef, recv_tables,
):
    gx, gy = lax.axis_index("gx"), lax.axis_index("gy")
    devices = groups * planes
    length = P_SIZE * Q
    pairs = HALF // groups
    chunks = pairs // STEP
    halves = pairs // EIGHT
    own = x_ref.shape[0]
    width = 2 * STEP
    block = Q // groups

    tables = [
        pltpu.make_async_copy(first_hbm, first_ref, recv_tables.at[0]),
        pltpu.make_async_copy(second_hbm, second_ref, recv_tables.at[1]),
    ]
    barrier = pltpu.get_barrier_semaphore()

    def target(offset):
        return jnp.bitwise_xor(gx, offset // planes), jnp.bitwise_xor(gy, offset % planes)

    def greet(offset, carry):
        pl.semaphore_signal(barrier, inc=1, device_id=target(offset), device_id_type=MESH)
        return carry

    lax.fori_loop(1, devices, greet, 0)
    pl.semaphore_wait(barrier, devices - 1)

    first_place = (gx * planes + gy) * own

    def row_copies(chunk, gxd, gyd):
        low = pl.multiple_of((gxd * pairs + chunk * STEP) * 2, width)
        high = pl.multiple_of(2 * Q - (gxd * pairs + (chunk + 1) * STEP) * 2, width)
        columns = pl.ds(pl.multiple_of(gyd * LANES, LANES), LANES)
        for side, at in ((0, low), (1, high)):
            yield (
                x_ref.at[:, pl.ds(at, width), columns],
                got_rows.at[chunk, pl.ds(first_place, own), pl.ds(side * width, width), :],
            )

    def send_chunk(chunk, carry):
        for source, place in row_copies(chunk, gx, gy):
            pltpu.make_async_copy(source, place, recv_rows.at[chunk]).start()

        def send(offset, carry):
            gxd, gyd = target(offset)
            for source, place in row_copies(chunk, gxd, gyd):
                pltpu.make_async_remote_copy(
                    src_ref=source, dst_ref=place, send_sem=send_rows,
                    recv_sem=recv_rows.at[chunk], device_id=(gxd, gyd), device_id_type=MESH,
                ).start()
            return carry

        lax.fori_loop(1, devices, send, 0)
        return carry

    lax.fori_loop(0, chunks, send_chunk, 0)
    for table in tables:
        table.start()

    slot_row = lax.broadcasted_iota(jnp.int32, (HALF, LANES), 0)

    def turn_table(at, carry):
        chunk, inner = at // width, at % width
        base = gx * pairs + chunk * STEP
        q = jnp.where(inner < STEP, base + inner, Q - 1 - (base + inner - STEP))
        angle = (slot_row * q).astype(jnp.float32) * (2 * math.pi / length)
        turn_cos[at] = jnp.cos(angle)
        turn_sin[at] = jnp.sin(angle)
        return carry

    lax.fori_loop(0, 2 * pairs, turn_table, 0)
    k2_row = lax.broadcasted_iota(jnp.int32, (Q, LANES), 0)
    end_angle = k2_row.astype(jnp.float32) * (math.pi * P_SIZE / (2 * length))
    factor = math.sqrt(2.0 / length)
    end_cos[...] = factor * jnp.cos(end_angle)
    end_sin[...] = factor * jnp.sin(end_angle)

    for table in tables:
        table.wait()

    def first_stage(chunk, carry):
        rows = got_rows.at[chunk]
        pltpu.make_async_copy(rows, rows, recv_rows.at[chunk]).wait()
        flat = rows.reshape(HALF * 2 * width, LANES)

        def line(row):
            return flat[pl.ds(row, HALF, stride=2 * width), :]

        for i in range(STEP):
            mirror = width + 2 * (STEP - 1 - i)
            value = jnp.concatenate(
                [
                    jnp.concatenate([line(2 * i), line(mirror)], axis=1),
                    jnp.concatenate([line(mirror + 1), line(2 * i + 1)], axis=1),
                ],
                axis=0,
            )
            both = three_dots(first_ref[0], first_ref[1], value)
            for side in range(2):
                inner = side * STEP + i
                real = both[:HALF, side * LANES : (side + 1) * LANES]
                imag = both[HALF:, side * LANES : (side + 1) * LANES]
                cos = turn_cos[chunk * width + inner]
                sin = turn_sin[chunk * width + inner]
                turned = real * cos + imag * sin, imag * cos - real * sin
                for plane in range(2):
                    parted = turned[plane].reshape(groups, halves, EIGHT, LANES)
                    for half in range(halves):
                        part[chunk, half, :, inner, plane] = parted[:, half]

        for half in range(halves):
            pltpu.make_async_copy(
                part.at[chunk, half, gx], got_part.at[half, gx, chunk], recv_part.at[half]
            ).start()
            for offset in range(1, groups):
                other = jnp.bitwise_xor(gx, offset)
                pltpu.make_async_remote_copy(
                    src_ref=part.at[chunk, half, other], dst_ref=got_part.at[half, gx, chunk],
                    send_sem=send_part, recv_sem=recv_part.at[half],
                    device_id=(other, gy), device_id_type=MESH,
                ).start()
        return carry

    lax.fori_loop(0, chunks, first_stage, 0)

    flat_coef = coef.reshape(2 * Q * pairs, LANES)

    def second_stage(half, within, carry):
        slot = half * EIGHT + within
        flat_part = got_part.at[half].reshape(Q * 2 * EIGHT, LANES)
        value = jnp.concatenate(
            [
                flat_part[pl.ds(plane * EIGHT + within, Q, stride=2 * EIGHT), :]
                for plane in range(2)
            ],
            axis=1,
        )
        frequency = gx * pairs + slot
        alone = frequency == 0
        which = jnp.where(alone, 1, 0)
        product = three_dots(second_ref[which, 0], second_ref[which, 1], value)
        top_real, top_imag = product[:Q, :LANES], product[:Q, LANES:]
        low_real, low_imag = product[Q:, :LANES], product[Q:, LANES:]
        spec_real = top_real + low_imag
        spec_imag = top_imag - low_real
        angle = jnp.full((8, LANES), frequency, jnp.int32).astype(jnp.float32) * (
            math.pi / (2 * length)
        )
        cos_one, sin_one = jnp.cos(angle)[:1], jnp.sin(angle)[:1]
        cos = end_cos[...] * cos_one - end_sin[...] * sin_one
        sin = end_sin[...] * cos_one + end_cos[...] * sin_one
        near = jnp.where(alone, top_real, cos * spec_real + sin * spec_imag)
        far = jnp.where(alone, low_imag, sin * spec_real - cos * spec_imag)
        flat_coef[pl.ds(slot, Q, stride=pairs), :] = near
        flat_coef[pl.ds(Q * pairs + pairs - 1 - slot, Q, stride=pairs), :] = far
        return carry

    def coef_copies(step, other):
        near = step * EIGHT
        far = pairs - EIGHT - near
        yield (
            coef.at[0, pl.ds(pl.multiple_of(other * block, block), block), pl.ds(near, EIGHT)],
            out_ref.at[0, :, pl.ds(pl.multiple_of(gx * pairs + near, EIGHT), EIGHT)],
        )
        away = groups - 1 - other
        yield (
            coef.at[1, pl.ds(pl.multiple_of(away * block, block), block), pl.ds(far, EIGHT)],
            out_ref.at[1, :, pl.ds(pl.multiple_of((groups - 1 - gx) * pairs + far, EIGHT), EIGHT)],
        )

    for step in range(halves):
        arrived = got_part.at[step]
        pltpu.make_async_copy(arrived, arrived, recv_part.at[step]).wait()
        lax.fori_loop(0, EIGHT, functools.partial(second_stage, step), 0)
        for source, place in coef_copies(step, gx):
            pltpu.make_async_copy(source, place, recv_coef).start()
        for offset in range(1, groups):
            other = jnp.bitwise_xor(gx, offset)
            for source, place in coef_copies(step, other):
                pltpu.make_async_remote_copy(
                    src_ref=source, dst_ref=place, send_sem=send_coef, recv_sem=recv_coef,
                    device_id=(other, gy), device_id_type=MESH,
                ).start()

    pltpu.make_async_copy(out_ref, out_ref, recv_coef).wait()
    sent = x_ref.at[:, pl.ds(0, 2 * Q - 2 * Q // devices), :]
    pltpu.make_async_copy(sent, sent, send_rows).wait()
    sent = part.at[:, :, pl.ds(0, groups - 1)]
    pltpu.make_async_copy(sent, sent, send_part).wait()
    sent = coef.at[:, pl.ds(0, Q - block)]
    pltpu.make_async_copy(sent, sent, send_coef).wait()


def fused_body(field):
    groups, planes = lax.axis_size("gx"), lax.axis_size("gy")
    pairs = HALF // groups
    chunks = pairs // STEP
    halves = pairs // EIGHT
    block = Q // groups
    own = field.shape[0] // (2 * Q)
    width = 2 * STEP
    f32 = jnp.float32
    vmem = pl.BlockSpec(memory_space=pltpu.VMEM)
    hbm = pl.BlockSpec(memory_space=pltpu.HBM)
    bf16 = jnp.bfloat16
    dma = pltpu.SemaphoreType.DMA
    both = pl.pallas_call(
        functools.partial(kernel, groups, planes),
        out_shape=jax.ShapeDtypeStruct((2, block, HALF, LANES), f32),
        in_specs=[pl.BlockSpec(memory_space=pl.ANY), hbm, hbm],
        out_specs=vmem,
        scratch_shapes=[
            pltpu.VMEM((2, P_SIZE, P_SIZE), bf16),
            pltpu.VMEM((2, 2, 2 * Q, Q), bf16),
            pltpu.VMEM((chunks, HALF, 2 * width, LANES), f32),
            pltpu.VMEM((chunks, halves, groups, width, 2, EIGHT, LANES), f32),
            pltpu.VMEM((halves, groups, chunks, width, 2, EIGHT, LANES), f32),
            pltpu.VMEM((2, Q, pairs, LANES), f32),
            pltpu.VMEM((2 * pairs, HALF, LANES), f32),
            pltpu.VMEM((2 * pairs, HALF, LANES), f32),
            pltpu.VMEM((Q, LANES), f32),
            pltpu.VMEM((Q, LANES), f32),
            dma((chunks,)), dma, dma((halves,)), dma, dma, dma, dma((2,)),
        ],
        compiler_params=pltpu.CompilerParams(
            collective_id=0, has_side_effects=True, vmem_limit_bytes=48 * 1024 * 1024
        ),
    )(
        field.reshape(own, 2 * Q, field.shape[1]),
        jnp.asarray(first_matrix()),
        jnp.asarray(second_matrices(groups)),
    )
    far = both[1, ::-1]
    result = jnp.concatenate([both[0], far[:, HALF - 1 :], far[:, : HALF - 1]], axis=1)
    return result.reshape(block * P_SIZE, LANES)


def fits(mesh):
    groups, planes = mesh.shape["gx"], mesh.shape["gy"]
    pairs = HALF // groups
    powers = groups & (groups - 1) == 0 and planes & (planes - 1) == 0
    return powers and pairs % 8 == 0 and (P_SIZE * Q) % (groups * planes * 2 * Q) == 0


def solution(mesh):
    in_specs = (P(("gx", "gy"), None),)
    out_specs = P("gx", "gy")
    def run(field):
        fused = fits(mesh) and field.shape[1] == LANES * mesh.shape["gy"]
        chosen = fused_body if fused else body
        return jax.shard_map(
            chosen, mesh=mesh, in_specs=in_specs, out_specs=out_specs, check_vma=False
        )(field)
    return run
```

```python
import functools
import math

import jax
import jax.numpy as jnp
from jax import lax
from jax.experimental import pallas as pl
from jax.experimental.pallas import tpu as pltpu
from jax.sharding import PartitionSpec as P

P_SIZE = 256
Q = 256
HALF = P_SIZE // 2
LANES = 128
STEP = 4
EIGHT = 8

MESH = pl.DeviceIdType.MESH
highest = lax.Precision.HIGHEST


def mat_dot(left, right):
    return jnp.dot(left, right, precision=highest, preferred_element_type=jnp.float32)


def finish(spec_real, spec_imag, frequency):
    length = P_SIZE * Q
    phases = math.pi / (2.0 * length) * frequency.astype(jnp.float32)
    factor = math.sqrt(2.0 / length)
    return factor * (
        jnp.cos(phases)[:, :, None] * spec_real + jnp.sin(phases)[:, :, None] * spec_imag
    )


def body(field):
    groups = lax.axis_size("gx")
    position = lax.axis_index("gx")
    length = P_SIZE * Q
    joined = lax.all_to_all(field, "gy", split_axis=1, concat_axis=0, tiled=True)
    row_count = joined.shape[0]
    col_width = joined.shape[1]
    half_rows = P_SIZE // (2 * groups)
    local_q = Q // groups
    local_p = P_SIZE // groups
    paired = joined.reshape(row_count // 2, 2, col_width)
    even_rows = paired[:, 0].reshape(half_rows, Q, col_width)
    odd_rows = jnp.flip(paired[:, 1].reshape(half_rows, Q, col_width), axis=1)
    low_half, high_half = (
        lax.all_to_all(even_rows, "gx", split_axis=1, concat_axis=0, tiled=True),
        lax.all_to_all(odd_rows, "gx", split_axis=1, concat_axis=0, tiled=True),
    )
    freq_first = jnp.arange(P_SIZE, dtype=jnp.int32)
    place_low = jnp.arange(P_SIZE // 2, dtype=jnp.int32)
    place_high = P_SIZE - 1 - place_low
    two_pi = 2.0 * math.pi
    low_phase = (
        two_pi / P_SIZE * (freq_first[:, None] * place_low[None, :] % P_SIZE).astype(jnp.float32)
    )
    high_phase = (
        two_pi / P_SIZE * (freq_first[:, None] * place_high[None, :] % P_SIZE).astype(jnp.float32)
    )
    flat_low = low_half.reshape(P_SIZE // 2, local_q * col_width)
    flat_high = high_half.reshape(P_SIZE // 2, local_q * col_width)
    cos_part = (
        mat_dot(jnp.cos(low_phase), flat_low) + mat_dot(jnp.cos(high_phase), flat_high)
    ).reshape(P_SIZE, local_q, col_width)
    sin_part = (
        mat_dot(jnp.sin(low_phase), flat_low) + mat_dot(jnp.sin(high_phase), flat_high)
    ).reshape(P_SIZE, local_q, col_width)
    part_imag = -sin_part
    second_place = position * local_q + jnp.arange(local_q, dtype=jnp.int32)
    turn_phase = (
        two_pi / length * (freq_first[:, None] * second_place[None, :] % length).astype(jnp.float32)
    )
    turn_cos = jnp.cos(turn_phase)[:, :, None]
    turn_sin = jnp.sin(turn_phase)[:, :, None]
    turned_real = cos_part * turn_cos + part_imag * turn_sin
    turned_imag = part_imag * turn_cos - cos_part * turn_sin
    moved_real, moved_imag = (
        lax.all_to_all(turned_real, "gx", split_axis=0, concat_axis=1, tiled=True),
        lax.all_to_all(turned_imag, "gx", split_axis=0, concat_axis=1, tiled=True),
    )
    second_index = jnp.arange(Q, dtype=jnp.int32)
    row_phase = two_pi / Q * (second_index[:, None] * second_index[None, :] % Q).astype(jnp.float32)
    row_cos = jnp.cos(row_phase)
    row_sin = jnp.sin(row_phase)
    spec_real = jnp.einsum("jb,kbc->jkc", row_cos, moved_real, precision=highest) + jnp.einsum(
        "jb,kbc->jkc", row_sin, moved_imag, precision=highest
    )
    spec_imag = jnp.einsum("jb,kbc->jkc", row_cos, moved_imag, precision=highest) - jnp.einsum(
        "jb,kbc->jkc", row_sin, moved_real, precision=highest
    )
    block_rows = lax.dynamic_slice_in_dim(freq_first, position * local_p, local_p, 0)
    frequency = block_rows[None, :] + P_SIZE * second_index[:, None]
    result = finish(spec_real, spec_imag, frequency)
    arrived = lax.all_to_all(result, "gx", split_axis=0, concat_axis=1, tiled=True)
    return arrived.reshape(local_q * P_SIZE, col_width)


def split(value):
    high = value.astype(jnp.bfloat16)
    low = (value - high.astype(jnp.float32)).astype(jnp.bfloat16)
    return high, low


def three_dots(high, low, value):
    value_high, value_low = split(value)
    dot = functools.partial(jnp.dot, preferred_element_type=jnp.float32)
    return dot(high, value_high) + (dot(high, value_low) + dot(low, value_high))


def kernel(
    groups, planes, x_ref, out_ref, first_ref, second_ref,
    got_rows, part, got_part, coef, turn_cos, turn_sin, end_cos, end_sin,
    recv_rows, send_rows, recv_part, send_part, recv_coef, send_coef,
):
    gx, gy = lax.axis_index("gx"), lax.axis_index("gy")
    devices = groups * planes
    length = P_SIZE * Q
    pairs = HALF // groups
    chunks = pairs // STEP
    halves = pairs // EIGHT
    own = x_ref.shape[0]
    width = 2 * STEP
    block = Q // groups

    barrier = pltpu.get_barrier_semaphore()

    def target(offset):
        return jnp.bitwise_xor(gx, offset // planes), jnp.bitwise_xor(gy, offset % planes)

    def greet(offset, carry):
        pl.semaphore_signal(barrier, inc=1, device_id=target(offset), device_id_type=MESH)
        return carry

    lax.fori_loop(1, devices, greet, 0)
    pl.semaphore_wait(barrier, devices - 1)

    first_place = (gx * planes + gy) * own

    def row_copies(chunk, gxd, gyd):
        low = pl.multiple_of((gxd * pairs + chunk * STEP) * 2, width)
        high = pl.multiple_of(2 * Q - (gxd * pairs + (chunk + 1) * STEP) * 2, width)
        columns = pl.ds(pl.multiple_of(gyd * LANES, LANES), LANES)
        for side, at in ((0, low), (1, high)):
            yield (
                x_ref.at[:, pl.ds(at, width), columns],
                got_rows.at[chunk, pl.ds(first_place, own), pl.ds(side * width, width), :],
            )

    def send_chunk(chunk, carry):
        for source, place in row_copies(chunk, gx, gy):
            pltpu.make_async_copy(source, place, recv_rows.at[chunk]).start()

        def send(offset, carry):
            gxd, gyd = target(offset)
            for source, place in row_copies(chunk, gxd, gyd):
                pltpu.make_async_remote_copy(
                    src_ref=source, dst_ref=place, send_sem=send_rows,
                    recv_sem=recv_rows.at[chunk], device_id=(gxd, gyd), device_id_type=MESH,
                ).start()
            return carry

        lax.fori_loop(1, devices, send, 0)
        return carry

    lax.fori_loop(0, chunks, send_chunk, 0)

    def iota(rows, columns, dimension):
        return lax.broadcasted_iota(jnp.int32, (rows, columns), dimension)

    def angles(steps, period):
        return (steps & (period - 1)).astype(jnp.float32) * (2 * math.pi / period)

    frequency_row, column = iota(HALF, P_SIZE, 0), iota(HALF, P_SIZE, 1)
    place = jnp.where(column < HALF, column, P_SIZE - 1 - (column - HALF))
    angle = angles(frequency_row * place, P_SIZE)
    middle = 1.0 - 2.0 * (place & 1).astype(jnp.float32)
    first_real, first_imag = jnp.cos(angle), jnp.where(frequency_row == 0, middle, -jnp.sin(angle))
    first_ref[0, :HALF], first_ref[1, :HALF] = split(first_real)
    first_ref[0, HALF:], first_ref[1, HALF:] = split(first_imag)

    k2, index = iota(Q, Q, 0), iota(Q, Q, 1)
    inner = index & (width - 1)
    base = (index >> (width.bit_length() - 1)) * STEP
    q = jnp.where(inner < STEP, base + inner, Q - 1 - (base + inner - STEP))
    angle = angles(k2 * q, Q)
    amplitude = math.sqrt(2.0 / length)
    for which, half, table in (
        (0, 0, jnp.cos(angle)),
        (0, 1, jnp.sin(angle)),
        (1, 0, amplitude * jnp.cos(angles(P_SIZE * k2 * (4 * q + 1), 4 * length))),
        (1, 1, amplitude * jnp.cos(
            angles((HALF + P_SIZE * (Q - 1 - k2)) * (4 * q + 1), 4 * length)
        )),
    ):
        high, low = split(table)
        second_ref[which, 0, half * Q : (half + 1) * Q] = high
        second_ref[which, 1, half * Q : (half + 1) * Q] = low

    slot_row = lax.broadcasted_iota(jnp.int32, (HALF, LANES), 0)

    def turn_table(at, carry):
        chunk, inner = at // width, at % width
        base = gx * pairs + chunk * STEP
        q = jnp.where(inner < STEP, base + inner, Q - 1 - (base + inner - STEP))
        angle = (slot_row * q).astype(jnp.float32) * (2 * math.pi / length)
        turn_cos[at] = jnp.cos(angle)
        turn_sin[at] = jnp.sin(angle)
        return carry

    lax.fori_loop(0, 2 * pairs, turn_table, 0)
    k2_row = lax.broadcasted_iota(jnp.int32, (Q, LANES), 0)
    end_angle = k2_row.astype(jnp.float32) * (math.pi * P_SIZE / (2 * length))
    factor = math.sqrt(2.0 / length)
    end_cos[...] = factor * jnp.cos(end_angle)
    end_sin[...] = factor * jnp.sin(end_angle)

    def first_stage(chunk, carry):
        rows = got_rows.at[chunk]
        pltpu.make_async_copy(rows, rows, recv_rows.at[chunk]).wait()
        flat = rows.reshape(HALF * 2 * width, LANES)

        def line(row):
            return flat[pl.ds(row, HALF, stride=2 * width), :]

        for i in range(STEP):
            mirror = width + 2 * (STEP - 1 - i)
            value = jnp.concatenate(
                [
                    jnp.concatenate([line(2 * i), line(mirror)], axis=1),
                    jnp.concatenate([line(mirror + 1), line(2 * i + 1)], axis=1),
                ],
                axis=0,
            )
            both = three_dots(first_ref[0], first_ref[1], value)
            for side in range(2):
                inner = side * STEP + i
                real = both[:HALF, side * LANES : (side + 1) * LANES]
                imag = both[HALF:, side * LANES : (side + 1) * LANES]
                cos = turn_cos[chunk * width + inner]
                sin = turn_sin[chunk * width + inner]
                turned = real * cos + imag * sin, imag * cos - real * sin
                for plane in range(2):
                    parted = turned[plane].reshape(groups, halves, EIGHT, LANES)
                    for half in range(halves):
                        part[chunk, half, :, inner, plane] = parted[:, half]

        for half in range(halves):
            pltpu.make_async_copy(
                part.at[chunk, half, gx], got_part.at[half, gx, chunk], recv_part.at[half]
            ).start()
            for offset in range(1, groups):
                other = jnp.bitwise_xor(gx, offset)
                pltpu.make_async_remote_copy(
                    src_ref=part.at[chunk, half, other], dst_ref=got_part.at[half, gx, chunk],
                    send_sem=send_part, recv_sem=recv_part.at[half],
                    device_id=(other, gy), device_id_type=MESH,
                ).start()
        return carry

    lax.fori_loop(0, chunks, first_stage, 0)

    flat_coef = coef.reshape(2 * Q * pairs, LANES)

    def second_stage(half, within, carry):
        slot = half * EIGHT + within
        flat_part = got_part.at[half].reshape(Q * 2 * EIGHT, LANES)
        value = jnp.concatenate(
            [
                flat_part[pl.ds(plane * EIGHT + within, Q, stride=2 * EIGHT), :]
                for plane in range(2)
            ],
            axis=1,
        )
        frequency = gx * pairs + slot
        alone = frequency == 0
        which = jnp.where(alone, 1, 0)
        product = three_dots(second_ref[which, 0], second_ref[which, 1], value)
        top_real, top_imag = product[:Q, :LANES], product[:Q, LANES:]
        low_real, low_imag = product[Q:, :LANES], product[Q:, LANES:]
        spec_real = top_real + low_imag
        spec_imag = top_imag - low_real
        angle = jnp.full((8, LANES), frequency, jnp.int32).astype(jnp.float32) * (
            math.pi / (2 * length)
        )
        cos_one, sin_one = jnp.cos(angle)[:1], jnp.sin(angle)[:1]
        cos = end_cos[...] * cos_one - end_sin[...] * sin_one
        sin = end_sin[...] * cos_one + end_cos[...] * sin_one
        near = jnp.where(alone, top_real, cos * spec_real + sin * spec_imag)
        far = jnp.where(alone, low_imag, sin * spec_real - cos * spec_imag)
        flat_coef[pl.ds(slot, Q, stride=pairs), :] = near
        flat_coef[pl.ds(Q * pairs + pairs - 1 - slot, Q, stride=pairs), :] = far
        return carry

    def coef_copies(step, other):
        near = step * EIGHT
        far = pairs - EIGHT - near
        yield (
            coef.at[0, pl.ds(pl.multiple_of(other * block, block), block), pl.ds(near, EIGHT)],
            out_ref.at[0, :, pl.ds(pl.multiple_of(gx * pairs + near, EIGHT), EIGHT)],
        )
        away = groups - 1 - other
        yield (
            coef.at[1, pl.ds(pl.multiple_of(away * block, block), block), pl.ds(far, EIGHT)],
            out_ref.at[1, :, pl.ds(pl.multiple_of((groups - 1 - gx) * pairs + far, EIGHT), EIGHT)],
        )

    for step in range(halves):
        arrived = got_part.at[step]
        pltpu.make_async_copy(arrived, arrived, recv_part.at[step]).wait()
        lax.fori_loop(0, EIGHT, functools.partial(second_stage, step), 0)
        for source, place in coef_copies(step, gx):
            pltpu.make_async_copy(source, place, recv_coef).start()
        for offset in range(1, groups):
            other = jnp.bitwise_xor(gx, offset)
            for source, place in coef_copies(step, other):
                pltpu.make_async_remote_copy(
                    src_ref=source, dst_ref=place, send_sem=send_coef, recv_sem=recv_coef,
                    device_id=(other, gy), device_id_type=MESH,
                ).start()

    pltpu.make_async_copy(out_ref, out_ref, recv_coef).wait()
    sent = x_ref.at[:, pl.ds(0, 2 * Q - 2 * Q // devices), :]
    pltpu.make_async_copy(sent, sent, send_rows).wait()
    sent = part.at[:, :, pl.ds(0, groups - 1)]
    pltpu.make_async_copy(sent, sent, send_part).wait()
    sent = coef.at[:, pl.ds(0, Q - block)]
    pltpu.make_async_copy(sent, sent, send_coef).wait()


def fused_body(field):
    groups, planes = lax.axis_size("gx"), lax.axis_size("gy")
    pairs = HALF // groups
    chunks = pairs // STEP
    halves = pairs // EIGHT
    block = Q // groups
    own = field.shape[0] // (2 * Q)
    width = 2 * STEP
    f32 = jnp.float32
    vmem = pl.BlockSpec(memory_space=pltpu.VMEM)
    bf16 = jnp.bfloat16
    dma = pltpu.SemaphoreType.DMA
    both = pl.pallas_call(
        functools.partial(kernel, groups, planes),
        out_shape=jax.ShapeDtypeStruct((2, block, HALF, LANES), f32),
        in_specs=[pl.BlockSpec(memory_space=pl.ANY)],
        out_specs=vmem,
        scratch_shapes=[
            pltpu.VMEM((2, P_SIZE, P_SIZE), bf16),
            pltpu.VMEM((2, 2, 2 * Q, Q), bf16),
            pltpu.VMEM((chunks, HALF, 2 * width, LANES), f32),
            pltpu.VMEM((chunks, halves, groups, width, 2, EIGHT, LANES), f32),
            pltpu.VMEM((halves, groups, chunks, width, 2, EIGHT, LANES), f32),
            pltpu.VMEM((2, Q, pairs, LANES), f32),
            pltpu.VMEM((2 * pairs, HALF, LANES), f32),
            pltpu.VMEM((2 * pairs, HALF, LANES), f32),
            pltpu.VMEM((Q, LANES), f32),
            pltpu.VMEM((Q, LANES), f32),
            dma((chunks,)), dma, dma((halves,)), dma, dma, dma,
        ],
        compiler_params=pltpu.CompilerParams(
            collective_id=0, has_side_effects=True, vmem_limit_bytes=48 * 1024 * 1024
        ),
    )(field.reshape(own, 2 * Q, field.shape[1]))
    far = both[1, ::-1]
    result = jnp.concatenate([both[0], far[:, HALF - 1 :], far[:, : HALF - 1]], axis=1)
    return result.reshape(block * P_SIZE, LANES)


def fits(mesh):
    groups, planes = mesh.shape["gx"], mesh.shape["gy"]
    pairs = HALF // groups
    powers = groups & (groups - 1) == 0 and planes & (planes - 1) == 0
    return powers and pairs % 8 == 0 and (P_SIZE * Q) % (groups * planes * 2 * Q) == 0


def solution(mesh):
    in_specs = (P(("gx", "gy"), None),)
    out_specs = P("gx", "gy")
    def run(field):
        fused = fits(mesh) and field.shape[1] == LANES * mesh.shape["gy"]
        chosen = fused_body if fused else body
        return jax.shard_map(
            chosen, mesh=mesh, in_specs=in_specs, out_specs=out_specs, check_vma=False
        )(field)
    return run
```

```python
import functools
import math

import jax
import jax.numpy as jnp
from jax import lax
from jax.experimental import pallas as pl
from jax.experimental.pallas import tpu as pltpu
from jax.sharding import PartitionSpec as P

P_SIZE = 256
Q = 256
HALF = P_SIZE // 2
LANES = 128
STEP = 4
EIGHT = 8

MESH = pl.DeviceIdType.MESH
highest = lax.Precision.HIGHEST


def mat_dot(left, right):
    return jnp.dot(left, right, precision=highest, preferred_element_type=jnp.float32)


def finish(spec_real, spec_imag, frequency):
    length = P_SIZE * Q
    phases = math.pi / (2.0 * length) * frequency.astype(jnp.float32)
    factor = math.sqrt(2.0 / length)
    return factor * (
        jnp.cos(phases)[:, :, None] * spec_real + jnp.sin(phases)[:, :, None] * spec_imag
    )


def body(field):
    groups = lax.axis_size("gx")
    position = lax.axis_index("gx")
    length = P_SIZE * Q
    joined = lax.all_to_all(field, "gy", split_axis=1, concat_axis=0, tiled=True)
    row_count = joined.shape[0]
    col_width = joined.shape[1]
    half_rows = P_SIZE // (2 * groups)
    local_q = Q // groups
    local_p = P_SIZE // groups
    paired = joined.reshape(row_count // 2, 2, col_width)
    even_rows = paired[:, 0].reshape(half_rows, Q, col_width)
    odd_rows = jnp.flip(paired[:, 1].reshape(half_rows, Q, col_width), axis=1)
    low_half, high_half = (
        lax.all_to_all(even_rows, "gx", split_axis=1, concat_axis=0, tiled=True),
        lax.all_to_all(odd_rows, "gx", split_axis=1, concat_axis=0, tiled=True),
    )
    freq_first = jnp.arange(P_SIZE, dtype=jnp.int32)
    place_low = jnp.arange(P_SIZE // 2, dtype=jnp.int32)
    place_high = P_SIZE - 1 - place_low
    two_pi = 2.0 * math.pi
    low_phase = (
        two_pi / P_SIZE * (freq_first[:, None] * place_low[None, :] % P_SIZE).astype(jnp.float32)
    )
    high_phase = (
        two_pi / P_SIZE * (freq_first[:, None] * place_high[None, :] % P_SIZE).astype(jnp.float32)
    )
    flat_low = low_half.reshape(P_SIZE // 2, local_q * col_width)
    flat_high = high_half.reshape(P_SIZE // 2, local_q * col_width)
    cos_part = (
        mat_dot(jnp.cos(low_phase), flat_low) + mat_dot(jnp.cos(high_phase), flat_high)
    ).reshape(P_SIZE, local_q, col_width)
    sin_part = (
        mat_dot(jnp.sin(low_phase), flat_low) + mat_dot(jnp.sin(high_phase), flat_high)
    ).reshape(P_SIZE, local_q, col_width)
    part_imag = -sin_part
    second_place = position * local_q + jnp.arange(local_q, dtype=jnp.int32)
    turn_phase = (
        two_pi / length * (freq_first[:, None] * second_place[None, :] % length).astype(jnp.float32)
    )
    turn_cos = jnp.cos(turn_phase)[:, :, None]
    turn_sin = jnp.sin(turn_phase)[:, :, None]
    turned_real = cos_part * turn_cos + part_imag * turn_sin
    turned_imag = part_imag * turn_cos - cos_part * turn_sin
    moved_real, moved_imag = (
        lax.all_to_all(turned_real, "gx", split_axis=0, concat_axis=1, tiled=True),
        lax.all_to_all(turned_imag, "gx", split_axis=0, concat_axis=1, tiled=True),
    )
    second_index = jnp.arange(Q, dtype=jnp.int32)
    row_phase = two_pi / Q * (second_index[:, None] * second_index[None, :] % Q).astype(jnp.float32)
    row_cos = jnp.cos(row_phase)
    row_sin = jnp.sin(row_phase)
    spec_real = jnp.einsum("jb,kbc->jkc", row_cos, moved_real, precision=highest) + jnp.einsum(
        "jb,kbc->jkc", row_sin, moved_imag, precision=highest
    )
    spec_imag = jnp.einsum("jb,kbc->jkc", row_cos, moved_imag, precision=highest) - jnp.einsum(
        "jb,kbc->jkc", row_sin, moved_real, precision=highest
    )
    block_rows = lax.dynamic_slice_in_dim(freq_first, position * local_p, local_p, 0)
    frequency = block_rows[None, :] + P_SIZE * second_index[:, None]
    result = finish(spec_real, spec_imag, frequency)
    arrived = lax.all_to_all(result, "gx", split_axis=0, concat_axis=1, tiled=True)
    return arrived.reshape(local_q * P_SIZE, col_width)


def split(value):
    high = value.astype(jnp.bfloat16)
    low = (value - high.astype(jnp.float32)).astype(jnp.bfloat16)
    return high, low


def three_dots(high, low, value):
    value_high, value_low = split(value)
    dot = functools.partial(jnp.dot, preferred_element_type=jnp.float32)
    return dot(high, value_high) + (dot(high, value_low) + dot(low, value_high))


def kernel(
    groups, planes, x_ref, out_ref, first_ref, second_ref,
    got_rows, part, got_part, coef, turn_cos, turn_sin, end_cos, end_sin,
    recv_rows, send_rows, recv_part, send_part, recv_coef, send_coef,
):
    gx, gy = lax.axis_index("gx"), lax.axis_index("gy")
    devices = groups * planes
    length = P_SIZE * Q
    pairs = HALF // groups
    chunks = pairs // STEP
    halves = pairs // EIGHT
    own = x_ref.shape[0]
    width = 2 * STEP
    block = Q // groups

    barrier = pltpu.get_barrier_semaphore()

    def target(offset):
        return jnp.bitwise_xor(gx, offset // planes), jnp.bitwise_xor(gy, offset % planes)

    def greet(offset, carry):
        pl.semaphore_signal(barrier, inc=1, device_id=target(offset), device_id_type=MESH)
        return carry

    lax.fori_loop(1, devices, greet, 0)
    pl.semaphore_wait(barrier, devices - 1)

    first_place = (gx * planes + gy) * own

    def row_copies(chunk, gxd, gyd):
        low = pl.multiple_of((gxd * pairs + chunk * STEP) * 2, width)
        high = pl.multiple_of(2 * Q - (gxd * pairs + (chunk + 1) * STEP) * 2, width)
        columns = pl.ds(pl.multiple_of(gyd * LANES, LANES), LANES)
        for side, at in ((0, low), (1, high)):
            yield (
                x_ref.at[:, pl.ds(at, width), columns],
                got_rows.at[chunk, pl.ds(first_place, own), pl.ds(side * width, width), :],
            )

    def send_chunk(chunk, carry):
        for source, place in row_copies(chunk, gx, gy):
            pltpu.make_async_copy(source, place, recv_rows.at[chunk]).start()

        def send(offset, carry):
            gxd, gyd = target(offset)
            for source, place in row_copies(chunk, gxd, gyd):
                pltpu.make_async_remote_copy(
                    src_ref=source, dst_ref=place, send_sem=send_rows,
                    recv_sem=recv_rows.at[chunk], device_id=(gxd, gyd), device_id_type=MESH,
                ).start()
            return carry

        lax.fori_loop(1, devices, send, 0)
        return carry

    lax.fori_loop(0, chunks, send_chunk, 0)

    def iota(rows, columns, dimension):
        return lax.broadcasted_iota(jnp.int32, (rows, columns), dimension)

    def angles(steps, period):
        return (steps & (period - 1)).astype(jnp.float32) * (2 * math.pi / period)

    frequency_row, column = iota(HALF, P_SIZE, 0), iota(HALF, P_SIZE, 1)
    place = jnp.where(column < HALF, column, P_SIZE - 1 - (column - HALF))
    angle = angles(frequency_row * place, P_SIZE)
    middle = 1.0 - 2.0 * (place & 1).astype(jnp.float32)
    first_real, first_imag = jnp.cos(angle), jnp.where(frequency_row == 0, middle, -jnp.sin(angle))
    first_ref[0, :HALF], first_ref[1, :HALF] = split(first_real)
    first_ref[0, HALF:], first_ref[1, HALF:] = split(first_imag)

    k2, index = iota(Q, Q, 0), iota(Q, Q, 1)
    inner = index & (width - 1)
    base = (index >> (width.bit_length() - 1)) * STEP
    q = jnp.where(inner < STEP, base + inner, Q - 1 - (base + inner - STEP))
    angle = angles(k2 * q, Q)
    amplitude = math.sqrt(2.0 / length)
    for which, half, table in (
        (0, 0, jnp.cos(angle)),
        (0, 1, jnp.sin(angle)),
        (1, 0, amplitude * jnp.cos(angles(P_SIZE * k2 * (4 * q + 1), 4 * length))),
        (1, 1, amplitude * jnp.cos(
            angles((HALF + P_SIZE * (Q - 1 - k2)) * (4 * q + 1), 4 * length)
        )),
    ):
        high, low = split(table)
        second_ref[which, 0, half * Q : (half + 1) * Q] = high
        second_ref[which, 1, half * Q : (half + 1) * Q] = low

    slot_row = lax.broadcasted_iota(jnp.int32, (HALF, LANES), 0)

    def turn_table(at, carry):
        chunk, inner = at // width, at % width
        base = gx * pairs + chunk * STEP
        q = jnp.where(inner < STEP, base + inner, Q - 1 - (base + inner - STEP))
        angle = (slot_row * q).astype(jnp.float32) * (2 * math.pi / length)
        turn_cos[at] = jnp.cos(angle)
        turn_sin[at] = jnp.sin(angle)
        return carry

    lax.fori_loop(0, 2 * pairs, turn_table, 0)
    k2_row = lax.broadcasted_iota(jnp.int32, (Q, LANES), 0)
    end_angle = k2_row.astype(jnp.float32) * (math.pi * P_SIZE / (2 * length))
    factor = math.sqrt(2.0 / length)
    end_cos[...] = factor * jnp.cos(end_angle)
    end_sin[...] = factor * jnp.sin(end_angle)

    def first_stage(chunk, carry):
        rows = got_rows.at[chunk]
        pltpu.make_async_copy(rows, rows, recv_rows.at[chunk]).wait()
        flat = rows.reshape(HALF * 2 * width, LANES)

        def line(row):
            return flat[pl.ds(row, HALF, stride=2 * width), :]

        for i in range(STEP):
            mirror = width + 2 * (STEP - 1 - i)
            value = jnp.concatenate(
                [
                    jnp.concatenate([line(2 * i), line(mirror)], axis=1),
                    jnp.concatenate([line(mirror + 1), line(2 * i + 1)], axis=1),
                ],
                axis=0,
            )
            both = three_dots(first_ref[0], first_ref[1], value)
            for side in range(2):
                inner = side * STEP + i
                real = both[:HALF, side * LANES : (side + 1) * LANES]
                imag = both[HALF:, side * LANES : (side + 1) * LANES]
                cos = turn_cos[chunk * width + inner]
                sin = turn_sin[chunk * width + inner]
                turned = real * cos + imag * sin, imag * cos - real * sin
                for plane in range(2):
                    parted = turned[plane].reshape(groups, halves, EIGHT, LANES)
                    for half in range(halves):
                        part[chunk, half, :, inner, plane] = parted[:, half]

        for half in range(halves):
            pltpu.make_async_copy(
                part.at[chunk, half, gx], got_part.at[half, gx, chunk], recv_part.at[half]
            ).start()
            for offset in (*range(2, groups, 2), *range(1, groups, 2)[1:], 1):
                other = jnp.bitwise_xor(gx, offset)
                pltpu.make_async_remote_copy(
                    src_ref=part.at[chunk, half, other], dst_ref=got_part.at[half, gx, chunk],
                    send_sem=send_part, recv_sem=recv_part.at[half],
                    device_id=(other, gy), device_id_type=MESH,
                ).start()
        return carry

    lax.fori_loop(0, chunks, first_stage, 0)

    flat_coef = coef.reshape(2 * Q * pairs, LANES)

    def second_stage(half, within, carry):
        slot = half * EIGHT + within
        flat_part = got_part.at[half].reshape(Q * 2 * EIGHT, LANES)
        value = jnp.concatenate(
            [
                flat_part[pl.ds(plane * EIGHT + within, Q, stride=2 * EIGHT), :]
                for plane in range(2)
            ],
            axis=1,
        )
        frequency = gx * pairs + slot
        alone = frequency == 0
        which = jnp.where(alone, 1, 0)
        product = three_dots(second_ref[which, 0], second_ref[which, 1], value)
        top_real, top_imag = product[:Q, :LANES], product[:Q, LANES:]
        low_real, low_imag = product[Q:, :LANES], product[Q:, LANES:]
        spec_real = top_real + low_imag
        spec_imag = top_imag - low_real
        angle = jnp.full((8, LANES), frequency, jnp.int32).astype(jnp.float32) * (
            math.pi / (2 * length)
        )
        cos_one, sin_one = jnp.cos(angle)[:1], jnp.sin(angle)[:1]
        cos = end_cos[...] * cos_one - end_sin[...] * sin_one
        sin = end_sin[...] * cos_one + end_cos[...] * sin_one
        near = jnp.where(alone, top_real, cos * spec_real + sin * spec_imag)
        far = jnp.where(alone, low_imag, sin * spec_real - cos * spec_imag)
        flat_coef[pl.ds(slot, Q, stride=pairs), :] = near
        flat_coef[pl.ds(Q * pairs + pairs - 1 - slot, Q, stride=pairs), :] = far
        return carry

    def coef_copies(step, other):
        near = step * EIGHT
        far = pairs - EIGHT - near
        yield (
            coef.at[0, pl.ds(pl.multiple_of(other * block, block), block), pl.ds(near, EIGHT)],
            out_ref.at[0, :, pl.ds(pl.multiple_of(gx * pairs + near, EIGHT), EIGHT)],
        )
        away = groups - 1 - other
        yield (
            coef.at[1, pl.ds(pl.multiple_of(away * block, block), block), pl.ds(far, EIGHT)],
            out_ref.at[1, :, pl.ds(pl.multiple_of((groups - 1 - gx) * pairs + far, EIGHT), EIGHT)],
        )

    for step in range(halves):
        arrived = got_part.at[step]
        pltpu.make_async_copy(arrived, arrived, recv_part.at[step]).wait()
        lax.fori_loop(0, EIGHT, functools.partial(second_stage, step), 0)
        for source, place in coef_copies(step, gx):
            pltpu.make_async_copy(source, place, recv_coef).start()
        for offset in (*range(2, groups, 2), *range(1, groups, 2)[1:], 1):
            other = jnp.bitwise_xor(gx, offset)
            for source, place in coef_copies(step, other):
                pltpu.make_async_remote_copy(
                    src_ref=source, dst_ref=place, send_sem=send_coef, recv_sem=recv_coef,
                    device_id=(other, gy), device_id_type=MESH,
                ).start()

    pltpu.make_async_copy(out_ref, out_ref, recv_coef).wait()
    sent = x_ref.at[:, pl.ds(0, 2 * Q - 2 * Q // devices), :]
    pltpu.make_async_copy(sent, sent, send_rows).wait()
    sent = part.at[:, :, pl.ds(0, groups - 1)]
    pltpu.make_async_copy(sent, sent, send_part).wait()
    sent = coef.at[:, pl.ds(0, Q - block)]
    pltpu.make_async_copy(sent, sent, send_coef).wait()


def fused_body(field):
    groups, planes = lax.axis_size("gx"), lax.axis_size("gy")
    pairs = HALF // groups
    chunks = pairs // STEP
    halves = pairs // EIGHT
    block = Q // groups
    own = field.shape[0] // (2 * Q)
    width = 2 * STEP
    f32 = jnp.float32
    vmem = pl.BlockSpec(memory_space=pltpu.VMEM)
    bf16 = jnp.bfloat16
    dma = pltpu.SemaphoreType.DMA
    both = pl.pallas_call(
        functools.partial(kernel, groups, planes),
        out_shape=jax.ShapeDtypeStruct((2, block, HALF, LANES), f32),
        in_specs=[pl.BlockSpec(memory_space=pl.ANY)],
        out_specs=vmem,
        scratch_shapes=[
            pltpu.VMEM((2, P_SIZE, P_SIZE), bf16),
            pltpu.VMEM((2, 2, 2 * Q, Q), bf16),
            pltpu.VMEM((chunks, HALF, 2 * width, LANES), f32),
            pltpu.VMEM((chunks, halves, groups, width, 2, EIGHT, LANES), f32),
            pltpu.VMEM((halves, groups, chunks, width, 2, EIGHT, LANES), f32),
            pltpu.VMEM((2, Q, pairs, LANES), f32),
            pltpu.VMEM((2 * pairs, HALF, LANES), f32),
            pltpu.VMEM((2 * pairs, HALF, LANES), f32),
            pltpu.VMEM((Q, LANES), f32),
            pltpu.VMEM((Q, LANES), f32),
            dma((chunks,)), dma, dma((halves,)), dma, dma, dma,
        ],
        compiler_params=pltpu.CompilerParams(
            collective_id=0, has_side_effects=True, vmem_limit_bytes=48 * 1024 * 1024
        ),
    )(field.reshape(own, 2 * Q, field.shape[1]))
    far = both[1, ::-1]
    result = jnp.concatenate([both[0], far[:, HALF - 1 :], far[:, : HALF - 1]], axis=1)
    return result.reshape(block * P_SIZE, LANES)


def fits(mesh):
    groups, planes = mesh.shape["gx"], mesh.shape["gy"]
    pairs = HALF // groups
    powers = groups & (groups - 1) == 0 and planes & (planes - 1) == 0
    return powers and pairs % 8 == 0 and (P_SIZE * Q) % (groups * planes * 2 * Q) == 0


def solution(mesh):
    in_specs = (P(("gx", "gy"), None),)
    out_specs = P("gx", "gy")
    def run(field):
        fused = fits(mesh) and field.shape[1] == LANES * mesh.shape["gy"]
        chosen = fused_body if fused else body
        return jax.shard_map(
            chosen, mesh=mesh, in_specs=in_specs, out_specs=out_specs, check_vma=False
        )(field)
    return run
```
